32 devices in a mesh: rows: 4 (over z), cx: 2 (over y), cy: 4 (over x, core).
Axes of the slice: x: 2, y: 2, z: 4, core: 2. Of those that a mesh axis runs over, the one named last changes fastest.
Arguments:
- rows_data: float32 [2048, 1024], P(('rows', 'cx', 'cy')), may hold values from -6 to 6
- owner_rows: int32 [2048, 1], P(('rows', 'cx', 'cy')), may hold values from 0 to 7; in each aligned block of 64 rows (0 to 63, 64 to 127, ...) at most 16 rows name the same one
- slot_rows: int32 [2048], P(('rows', 'cx', 'cy')), may hold values from 0 to 2047
- centroids: float32 [16384, 1024], P(('cx', 'cy'), 'rows'), may hold values from -6 to 6
- counts: float32 [16384], P(('cx', 'cy')), may hold values from 1 to 100
- owner_cent: int32 [16384, 1], P(('cx', 'cy')), may hold values from 0 to 7; in each aligned block of 2048 rows (0 to 2047, 2048 to 4095, ...) at most 512 rows name the same one
- slot_cent: int32 [16384], P(('cx', 'cy')), may hold values from 0 to 511
- upper: float32 [4096, 1024], P(('cx', 'cy'), 'rows'), may hold values from -6 to 6
- upper_counts: float32 [4096], P(('cx', 'cy')), may hold values from 1 to 100
Outputs:
- moved: float32 [16384, 1024], P(('cx', 'cy'), 'rows')
- new_counts: float32 [16384], P(('cx', 'cy'))
- new_upper: float32 [4096, 1024], P(('cx', 'cy'), 'rows')
- new_upper_counts: float32 [4096], P(('cx', 'cy'))
The draws below stay inside these ranges and needn't reach their ends.
Inputs may be any that keep to these rules, and one draw needn't show every extreme that they name: `owner_rows`: the rows of one device name each value at most 16 times, and some device reaches it. `owner_cent`: the 2048 level-1 centroids of one shard name each value at most 512 times, and some shard reaches it.
All inputs are finite; a program needn't handle non-finite values.
Results may differ from the reference program's by a relative error of at most 0.00002.
Values sent between devices are 32-bit elements; how exact they have to be, the bound alone decides.
A program may use at most 64 MiB of HBM per device.

```python
import math
import jax
import jax.numpy as jnp
import numpy as np

D = 1024
C1_DEV = 2048
K2 = 4096
TOK_DEV = 64
SHARDS = 8
C1 = 16384
K2_DEV = 512
ROWS_ALL = 2048
CAP1 = 16
CAP2 = 512


def plant(entries, rng, smallest, top_value):
    spot = [jax.random.randint(jax.random.fold_in(rng, axis), (), 0, length) for axis, length in enumerate(entries.shape)]
    main_axis = entries.shape.index(max(entries.shape))
    beside = spot[:main_axis] + [(spot[main_axis] + 1) % entries.shape[main_axis]] + spot[main_axis + 1:]
    return entries.at[tuple(spot)].set(smallest).at[tuple(beside)].set(top_value)


def block_levels(key, extent, split, least, high):
    gain, own = 1.0, jax.random.fold_in(key, 6)
    for dim, blocks in split:
        heights = jnp.exp(jax.random.uniform(jax.random.fold_in(own, dim), (blocks,), jnp.float32, least / len(split), high / len(split)))
        gain = gain * jnp.repeat(heights, extent[dim] // blocks).reshape([-1 if axis == dim else 1 for axis in range(len(extent))])
    return gain


def shared_out(key, own, number, rows, amount, top, limit, slope):
    ranking = jax.random.permutation(key, amount)
    heavy_load, ordinary = shares(amount, rows * top, limit, slope, True), shares(amount, rows * top, limit, slope, False)
    places = jnp.arange(amount)

    def named(lengths, offset_by):
        used = int((lengths > 0).sum())
        fixed = max(1, used // 4)
        passed = fixed + (places - fixed + offset_by * (used - fixed)) % max(1, amount - fixed)
        return jnp.zeros((amount,), jnp.int32).at[ranking[jnp.where(places < fixed, places, passed)]].set(jnp.asarray(lengths, jnp.int32))

    lengths = jnp.where(number % 4 == 0, named(heavy_load, number // 4), named(ordinary, number - number // 4 - 1))
    mixed = jax.random.permutation(jax.random.fold_in(own, 3), amount)
    giver, receiver = mixed[0:amount // 2 * 2:2], mixed[1:amount // 2 * 2:2]
    room = jnp.minimum(lengths[giver] - 1, limit - lengths[receiver]) // 2
    room = jnp.where((giver == ranking[0]) | (receiver == ranking[0]) | (lengths[receiver] == 0), 0, jnp.maximum(room, 0))
    passed = jax.random.randint(jax.random.fold_in(own, 4), (amount // 2,), 0, 1 << 20) % (room + 1)
    lengths = lengths.at[giver].add(-passed).at[receiver].add(passed)
    members = jnp.searchsorted(jnp.cumsum(lengths), jnp.arange(rows * top), side="right").astype(jnp.int32)
    listing = members.reshape(top, rows).T
    listing = listing[jax.random.permutation(jax.random.fold_in(own, 1), rows)]
    offset_by = jax.random.randint(jax.random.fold_in(own, 2), (rows, 1), 0, top)
    return jnp.take_along_axis(listing, (jnp.arange(top)[None, :] + offset_by) % top, axis=1)


def shares(count, total, bound, slope, full):
    weights = [(1 << 20) // math.isqrt(standing ** slope) + 1 for standing in range(1, count + 1)]
    largest = bound if full else min(bound, max(-(-total // count), total * weights[0] // sum(weights)))
    least = 1 if total - largest >= count - 1 else 0
    given, rest = [largest] + [least] * (count - 1), total - largest - least * (count - 1)
    while rest > 0:
        free = [i for i in range(1, count) if given[i] < largest] or [i for i in range(1, count) if given[i] < bound]
        mass, left = sum([weights[i] for i in free]), rest
        for i in free:
            extra = min(bound - given[i], max(1, left * weights[i] // mass), rest)
            given[i] = given[i] + extra
            rest = rest - extra
    return np.array(given)


def centred(stream_key, dims, deviation, reach, pieces=(), dtype=jnp.bfloat16):
    entries = jax.random.normal(stream_key, dims, jnp.float32) * deviation
    if len(pieces) > 0:
        entries = block_levels(stream_key, dims, pieces, -0.22, 0.18) * entries
    return jnp.clip(entries, min=-reach, max=reach).astype(dtype)


def setup_inputs(seed: int = 0) -> dict:
    arg_keys = jax.random.split(jax.random.key(seed), 10)
    rows_data = centred(arg_keys[0], (ROWS_ALL, D), 1.0, 6.0, ((0, 32),), jnp.float32)
    owner_rows_keys = jax.random.split(jax.random.fold_in(arg_keys[1], 1), ROWS_ALL // TOK_DEV)
    owner_rows_turns = jax.random.permutation(jax.random.fold_in(arg_keys[1], 3), ROWS_ALL // TOK_DEV)
    owner_rows = jax.vmap(lambda own, number: shared_out(jax.random.fold_in(arg_keys[1], 2), own, number, TOK_DEV, SHARDS, 1, CAP1, 2))(owner_rows_keys, owner_rows_turns).reshape((ROWS_ALL, 1))
    slot_rows = plant(jax.random.randint(arg_keys[2], (ROWS_ALL,), 0, C1_DEV), jax.random.fold_in(arg_keys[2], 1), 0, C1_DEV - 1).astype(jnp.int32)
    centroids = centred(arg_keys[3], (C1, D), 1.0, 6.0, ((0, 8), (1, 4)), jnp.float32)
    counts = jnp.clip(jnp.exp(math.log(100.0) - 4.6051702 * jax.random.uniform(arg_keys[4], (C1,), jnp.float32) ** block_levels(arg_keys[4], (C1,), ((0, 8),), -0.2, 0.2)), 1.0, 100.0)
    owner_cent_keys = jax.random.split(jax.random.fold_in(arg_keys[5], 1), C1 // C1_DEV)
    owner_cent_turns = jax.random.permutation(jax.random.fold_in(arg_keys[5], 3), C1 // C1_DEV)
    owner_cent = jax.vmap(lambda own, number: shared_out(jax.random.fold_in(arg_keys[5], 2), own, number, C1_DEV, SHARDS, 1, CAP2, 2))(owner_cent_keys, owner_cent_turns).reshape((C1, 1))
    slot_cent = plant(jax.random.randint(arg_keys[6], (C1,), 0, K2_DEV), jax.random.fold_in(arg_keys[6], 1), 0, K2_DEV - 1).astype(jnp.int32)
    upper = centred(arg_keys[7], (K2, D), 1.0, 6.0, ((0, 8), (1, 4)), jnp.float32)
    upper_counts = jnp.clip(jnp.exp(math.log(100.0) - 4.6051702 * jax.random.uniform(arg_keys[8], (K2,), jnp.float32) ** block_levels(arg_keys[8], (K2,), ((0, 8),), -0.2, 0.2)), 1.0, 100.0)
    return dict(rows_data=rows_data, owner_rows=owner_rows, slot_rows=slot_rows, centroids=centroids, counts=counts, owner_cent=owner_cent, slot_cent=slot_cent, upper=upper, upper_counts=upper_counts)


def reference(rows_data, owner_rows, slot_rows, centroids, counts, owner_cent, slot_cent, upper, upper_counts):
    lower_ids = owner_rows[:, 0] * C1_DEV + slot_rows
    summed = jax.ops.segment_sum(rows_data, lower_ids, num_segments=C1)
    member_counts = jax.ops.segment_sum(jnp.ones(lower_ids.shape, jnp.float32), lower_ids, num_segments=C1)
    new_counts = counts + member_counts
    moved = centroids + (summed - member_counts[:, None] * centroids) / new_counts[:, None]
    upper_ids = owner_cent[:, 0] * K2_DEV + slot_cent
    upper_summed = jax.ops.segment_sum(moved, upper_ids, num_segments=K2)
    upper_members = jax.ops.segment_sum(jnp.ones(upper_ids.shape, jnp.float32), upper_ids, num_segments=K2)
    new_upper_counts = upper_counts + upper_members
    new_upper = upper + (upper_summed - upper_members[:, None] * upper) / new_upper_counts[:, None]
    return moved, new_counts, new_upper, new_upper_counts
```

```python
import functools

import jax
import jax.numpy as jnp
from jax import lax
from jax.experimental import pallas as pl
from jax.experimental.pallas import tpu as pltpu
from jax.sharding import PartitionSpec as P

MESH = pl.DeviceIdType.MESH
LANES = 128
CORES = 2


def bucket(values, owners, slot_ids, shards, capacity, empty):
    onehot = (owners[:, None] == jnp.arange(shards, dtype=jnp.int32)[None, :]).astype(jnp.int32)
    earlier = jnp.cumsum(onehot, axis=0) - onehot
    position = jnp.sum(earlier * onehot, axis=1)
    target = owners * capacity + position
    buffer = jnp.zeros((shards * capacity, values.shape[1]), values.dtype).at[target].set(values)
    labels = jnp.full((shards * capacity,), empty, jnp.int32).at[target].set(slot_ids)
    return (buffer.reshape(shards, capacity, values.shape[1]), labels.reshape(shards, capacity))


def count_columns(ids_row, rows, base, limit):
    spots = lax.broadcasted_iota(jnp.int32, (limit, LANES), 0) + base

    def step(i, total):
        line = jnp.broadcast_to(ids_row(i), (limit, LANES))
        return total + jnp.where(line == spots, 1.0, 0.0)

    total = lax.fori_loop(0, rows, step, jnp.zeros((limit, LANES), jnp.float32))
    return jnp.sum(total, axis=1, keepdims=True)


def local_kernel(lower_s, upper_s, lower_v, data, cent, counts, moved, news, partial, summed, members):
    summed[...] = jnp.zeros_like(summed)
    partial[...] = jnp.zeros_like(partial)

    def add_row(i, _):
        spot = lower_s[i]
        summed[pl.ds(spot, 1), :] += data[pl.ds(i, 1), :]
        return 0

    lax.fori_loop(0, lower_s.shape[0], add_row, 0, unroll=8)
    block = min(LANES, cent.shape[0])

    def move(b, _):
        here = pl.ds(pl.multiple_of(b * block, block), block)
        m = count_columns(lambda i: lower_v[pl.ds(i, 1), :], lower_v.shape[0], b * block, block)
        n = counts[here, :] + m
        prev = cent[here, :]
        moved[here, :] = prev + (summed[here, :] - m * prev) / n[:, :1]
        news[here, :] = n
        return 0

    lax.fori_loop(0, cent.shape[0] // block, move, 0)

    def add_moved(i, _):
        spot = upper_s[i]
        partial[pl.ds(spot, 1), :] += moved[pl.ds(i, 1), :]
        return 0

    lax.fori_loop(0, upper_s.shape[0], add_moved, 0, unroll=8)


def local_update(labels, labels_upper, data, centroids, counts, slots):
    rows, width = centroids.shape
    vm = pl.BlockSpec(memory_space=pltpu.VMEM)
    sm = pl.BlockSpec(memory_space=pltpu.SMEM)
    return pl.pallas_call(
        local_kernel,
        out_shape=(
            jax.ShapeDtypeStruct((rows, width), jnp.float32),
            jax.ShapeDtypeStruct((rows, LANES), jnp.float32),
            jax.ShapeDtypeStruct((slots, width), jnp.float32),
        ),
        in_specs=[sm, sm, vm, vm, vm, vm],
        out_specs=(vm, vm, vm),
        scratch_shapes=[
            pltpu.VMEM((rows + 8, width), jnp.float32),
            pltpu.VMEM((rows, LANES), jnp.float32),
        ],
        compiler_params=pltpu.CompilerParams(vmem_limit_bytes=60 * 1024 * 1024),
        name="local_update",
    )(
        labels,
        labels_upper,
        labels.reshape(-1, LANES),
        data,
        centroids,
        jnp.broadcast_to(counts[:, None], (rows, LANES)),
    )


def reduce_kernel(
    ys, xs, part, ids, upper, weights, out, news,
    pair, chip, a1, b1, a2, b2, seen,
    s0, r0, sa1, ra1, sb1, rb1, sa2, ra2, sb2, rb2, si, ri,
):
    y = lax.axis_index("cx")
    cy = lax.axis_index("cy")
    x, core = lax.div(cy, CORES), lax.rem(cy, CORES)
    cys = xs * CORES
    shards = ys * cys
    me = y * cys + cy
    slots = part.shape[1]
    half = slots // 2
    lines = ids.shape[0]

    barrier = pltpu.get_barrier_semaphore()
    peers = []
    for d in range(1, shards):
        t = lax.rem(me + d, shards)
        peers.append({"cx": lax.div(t, cys), "cy": lax.rem(t, cys)})
    for peer in peers:
        pl.semaphore_signal(barrier, inc=1, device_id=peer, device_id_type=MESH)
    pl.semaphore_wait(barrier, shards - 1)

    def remote(src, dst, send, recv, peer):
        copy = pltpu.make_async_remote_copy(
            src_ref=src, dst_ref=dst, send_sem=send, recv_sem=recv, device_id=peer, device_id_type=MESH
        )
        copy.start()
        return copy

    offsets = [(dy, dx) for dy in range(ys) for dx in range(xs)]
    offsets.sort(key=lambda o: -((o[0] != 0) * 2 + (o[1] != 0) * 2))

    def at(dy, dx):
        return lax.rem(y + dy, ys), lax.rem(x + dx, xs)

    started = []
    first = {}
    for dy, dx in offsets:
        ty, tx = at(dy, dx)
        k = dy * xs + dx
        first[dy, dx] = remote(
            part.at[(ty * xs + tx) * CORES + 1 - core], pair.at[k], s0.at[k], r0.at[k],
            {"cx": y, "cy": x * CORES + 1 - core},
        )
    idc = [remote(ids, seen.at[d], si.at[d - 1], ri.at[d - 1], peers[d - 1]) for d in range(1, shards)]
    seen[0] = ids[...]

    ac, bc = {}, {}
    for dy, dx in offsets:
        ty, tx = at(dy, dx)
        k = dy * xs + dx
        first[dy, dx].wait_recv()
        chip[k] = part[(ty * xs + tx) * CORES + core] + pair[k]
        if dy:
            ac[dy, dx] = remote(
                chip.at[k, pl.ds(0, half)], a1.at[(dy - 1) * xs + dx],
                sa1.at[(dy - 1) * xs + dx], ra1.at[(dy - 1) * xs + dx],
                {"cx": ty, "cy": cy},
            )
        if dx:
            bc[dy, dx] = remote(
                chip.at[k, pl.ds(half, half)], b1.at[(dx - 1) * ys + dy],
                sb1.at[(dx - 1) * ys + dy], rb1.at[(dx - 1) * ys + dy],
                {"cx": y, "cy": tx * CORES + core},
            )

    a2c, b2c = {}, {}
    for dx in range(1, xs):
        for dy in range(1, ys):
            ac[dy, dx].wait_recv()
        total = chip[dx, :half]
        for dy in range(1, ys):
            total = total + a1[(dy - 1) * xs + dx]
        chip[dx, :half] = total
        a2c[dx] = remote(
            chip.at[dx, pl.ds(0, half)], a2.at[dx - 1], sa2.at[dx - 1], ra2.at[dx - 1],
            {"cx": y, "cy": lax.rem(x + dx, xs) * CORES + core},
        )
    for dy in range(1, ys):
        for dx in range(1, xs):
            bc[dy, dx].wait_recv()
        total = chip[dy * xs, half:]
        for dx in range(1, xs):
            total = total + b1[(dx - 1) * ys + dy]
        chip[dy * xs, half:] = total
        b2c[dy] = remote(
            chip.at[dy * xs, pl.ds(half, half)], b2.at[dy - 1], sb2.at[dy - 1], rb2.at[dy - 1],
            {"cx": lax.rem(y + dy, ys), "cy": cy},
        )

    for copy in idc:
        copy.wait_recv()
    block = min(LANES, slots)
    for b in range(slots // block):
        here = pl.ds(b * block, block)
        m = count_columns(
            lambda i: seen[lax.div(i, lines), pl.ds(lax.rem(i, lines), 1), :],
            shards * lines, me * slots + b * block, block,
        )
        n = weights[here, :] + m
        news[here, :] = n
        prev = upper[here, :]
        out[here, :] = m * prev

    for dy in range(1, ys):
        ac[dy, 0].wait_recv()
    for dx in range(1, xs):
        bc[0, dx].wait_recv()
    for dx in range(1, xs):
        a2c[dx].wait_recv()
    for dy in range(1, ys):
        b2c[dy].wait_recv()

    def close(rows, total):
        prev = upper[rows, :]
        out[rows, :] = prev + (total - out[rows, :]) / news[rows, :1]

    total = chip[0, :half]
    for dy in range(1, ys):
        total = total + a1[(dy - 1) * xs]
    for dx in range(1, xs):
        total = total + a2[dx - 1]
    close(pl.ds(0, half), total)
    total = chip[0, half:]
    for dx in range(1, xs):
        total = total + b1[(dx - 1) * ys]
    for dy in range(1, ys):
        total = total + b2[dy - 1]
    close(pl.ds(half, half), total)

    for group in (first.values(), idc, ac.values(), bc.values(), a2c.values(), b2c.values()):
        for copy in group:
            copy.wait_send()


def reduce_update(partial, ids, upper, weights, ys, xs):
    slots, width = upper.shape
    half = slots // 2
    shards = ys * xs * CORES
    vm = pl.BlockSpec(memory_space=pltpu.VMEM)
    f32 = jnp.float32
    n0, na, nb = ys * xs, (ys - 1) * xs, (xs - 1) * ys
    dma = lambda n: pltpu.SemaphoreType.DMA((n,))
    return pl.pallas_call(
        functools.partial(reduce_kernel, ys, xs),
        out_shape=(
            jax.ShapeDtypeStruct((slots, width), f32),
            jax.ShapeDtypeStruct((slots, LANES), f32),
        ),
        in_specs=[vm] * 4,
        out_specs=(vm, vm),
        scratch_shapes=[
            pltpu.VMEM((n0, slots, width), f32),
            pltpu.VMEM((n0, slots, width), f32),
            pltpu.VMEM((na, half, width), f32),
            pltpu.VMEM((nb, half, width), f32),
            pltpu.VMEM((xs - 1, half, width), f32),
            pltpu.VMEM((ys - 1, half, width), f32),
            pltpu.VMEM((shards,) + ids.shape, jnp.int32),
            dma(n0), dma(n0), dma(na), dma(na), dma(nb), dma(nb),
            dma(xs - 1), dma(xs - 1), dma(ys - 1), dma(ys - 1),
            dma(shards - 1), dma(shards - 1),
        ],
        compiler_params=pltpu.CompilerParams(
            collective_id=1, has_side_effects=True, vmem_limit_bytes=60 * 1024 * 1024
        ),
        name="reduce_update",
    )(
        partial.reshape(shards, slots, width),
        ids,
        upper,
        jnp.broadcast_to(weights[:, None], (slots, LANES)),
    )


def body(
    rows_data, owner_rows, slot_rows, centroids, counts, owner_cent, slot_cent, upper, upper_counts
):
    shards = lax.axis_size(("cx", "cy"))
    groups = lax.axis_size("rows")
    batch = rows_data.shape[0]
    lower_rows = centroids.shape[0]
    capacity = 2 * batch // shards
    buffer, labels = bucket(rows_data, owner_rows[:, 0], slot_rows, shards, capacity, lower_rows)
    labels = jnp.broadcast_to(labels[:, :, None], (shards, capacity, groups))
    arrived, arrived_labels = (
        lax.all_to_all(
            lax.all_to_all(buffer, "rows", split_axis=2, concat_axis=1, tiled=True),
            ("cx", "cy"),
            split_axis=0,
            concat_axis=0,
            tiled=True,
        ),
        lax.all_to_all(
            lax.all_to_all(labels, "rows", split_axis=2, concat_axis=1, tiled=True),
            ("cx", "cy"),
            split_axis=0,
            concat_axis=0,
            tiled=True,
        ),
    )
    slice_width = arrived.shape[2]
    upper_rows = upper.shape[0]
    ids = owner_cent[:, 0] * upper_rows + slot_cent
    moved, news, partial = local_update(
        arrived_labels.reshape(-1), ids, arrived.reshape(-1, slice_width), centroids, counts,
        upper_rows * shards,
    )
    ys, xs = lax.axis_size("cx"), lax.axis_size("cy") // CORES
    new_upper, new_weights = reduce_update(
        partial, ids.reshape(-1, LANES), upper, upper_counts, ys, xs
    )
    return (moved, news[:, 0], new_upper, new_weights[:, 0])
def solution(mesh):
    placed = (
        P(("rows", "cx", "cy"), None),
        P(("rows", "cx", "cy"), None),
        P(("rows", "cx", "cy")),
        P(("cx", "cy"), "rows"),
        P(("cx", "cy")),
        P(("cx", "cy"), None),
        P(("cx", "cy")),
        P(("cx", "cy"), "rows"),
        P(("cx", "cy")),
    )
    return jax.shard_map(
        body,
        mesh=mesh,
        in_specs=placed,
        out_specs=(
            P(("cx", "cy"), "rows"),
            P(("cx", "cy")),
            P(("cx", "cy"), "rows"),
            P(("cx", "cy")),
        ),
        check_vma=False,
    )
```

```python
import functools

import jax
import jax.numpy as jnp
from jax import lax
from jax.experimental import pallas as pl
from jax.experimental.pallas import tpu as pltpu
from jax.sharding import PartitionSpec as P

MESH = pl.DeviceIdType.MESH
LANES = 128
CORES = 2


def exchange_kernel(
    capacity, empty, rows_ref, owner_ref, slot_ref, data, labels,
    info, mine, slabs, packed, inbox, tags, heard,
    si, ri, ss, rs, sp, rp, st, rt,
):
    groups, batch, width = slabs.shape
    shards = inbox.shape[0]
    spots = shards * capacity
    z = lax.axis_index("rows")
    cys = lax.axis_size("cy")
    me = lax.axis_index("cx") * cys + lax.axis_index("cy")

    info[...] = jnp.full_like(info, -1)
    info[0:1, :batch] = owner_ref[...]
    info[1:2, :batch] = slot_ref[...]
    tags[...] = jnp.full_like(tags, empty)

    barrier = pltpu.get_barrier_semaphore()
    mates = [{"rows": lax.rem(z + d, groups)} for d in range(1, groups)]
    peers = []
    for d in range(1, shards):
        t = lax.rem(me + d, shards)
        peers.append({"cx": lax.div(t, cys), "cy": lax.rem(t, cys)})
    for peer in mates + peers:
        pl.semaphore_signal(barrier, inc=1, device_id=peer, device_id_type=MESH)
    pl.semaphore_wait(barrier, groups - 1 + shards - 1)

    def remote(src, dst, send, recv, peer):
        copy = pltpu.make_async_remote_copy(
            src_ref=src, dst_ref=dst, send_sem=send, recv_sem=recv, device_id=peer, device_id_type=MESH
        )
        copy.start()
        return copy

    def columns(group):
        return pl.ds(pl.multiple_of(group * width, width), width)

    asked = [remote(info, mine.at[d], si.at[d - 1], ri.at[d - 1], mates[d - 1]) for d in range(1, groups)]
    sent = [
        remote(
            rows_ref.at[:, columns(mates[d - 1]["rows"])], slabs.at[d],
            ss.at[d - 1], rs.at[d - 1], mates[d - 1],
        )
        for d in range(1, groups)
    ]
    mine[0] = info[...]
    slabs[0] = rows_ref[:, columns(z)]

    bf16, f32 = jnp.bfloat16, jnp.float32
    up = lax.broadcasted_iota(jnp.int32, (LANES, LANES), 0)
    across = lax.broadcasted_iota(jnp.int32, (LANES, LANES), 1)
    before = jnp.where(up < across, 1.0, 0.0).astype(bf16)
    shard_of = lax.broadcasted_iota(jnp.int32, (shards, LANES), 0)
    spot_of = lax.broadcasted_iota(jnp.int32, (spots, LANES), 0)
    line = lax.broadcasted_iota(jnp.int32, (8, LANES), 0)
    moves = []
    for d in range(groups):
        if d:
            asked[d - 1].wait_recv()
        owner, slot = mine[d, 0:1, :], mine[d, 1:2, :]
        named = jnp.where(jnp.broadcast_to(owner, (shards, LANES)) == shard_of, 1.0, 0.0)
        earlier = jnp.dot(named.astype(bf16), before, preferred_element_type=f32)
        position = jnp.sum(named * earlier, axis=0, keepdims=True).astype(jnp.int32)
        target = jnp.where(owner >= 0, owner * capacity + position, -1)
        pick = jnp.where(jnp.broadcast_to(target, (spots, LANES)) == spot_of, 1.0, 0.0).astype(bf16)
        high = jnp.broadcast_to(lax.shift_right_arithmetic(slot, 7), (8, LANES))
        low = jnp.broadcast_to(slot & 127, (8, LANES))
        code = jnp.where(line == 0, high, jnp.where(line == 1, low, 1)).astype(f32).astype(bf16)
        found = lax.dot_general(code, pick, (((1,), (1,)), ((), ())), preferred_element_type=f32)
        tag = (found[0:1] * 128.0 + found[1:2]).astype(jnp.int32)
        tags[d : d + 1, :] = jnp.where(found[2:3] > 0.5, tag, empty)
        if d:
            sent[d - 1].wait_recv()
        slab = slabs[d]
        first = slab.astype(bf16)
        left = slab - first.astype(f32)
        second = left.astype(bf16)
        third = (left - second.astype(f32)).astype(bf16)
        chosen = pick[:, :batch]
        total = jnp.dot(chosen, third, preferred_element_type=f32)
        total = total + jnp.dot(chosen, second, preferred_element_type=f32)
        packed[d] = total + jnp.dot(chosen, first, preferred_element_type=f32)
        for p in range(1, shards):
            t = lax.rem(me + p, shards)
            k = (p - 1) * groups + d
            moves.append(
                remote(
                    packed.at[d, pl.ds(pl.multiple_of(t * capacity, 8), capacity)], inbox.at[p, d],
                    sp.at[k], rp.at[k], peers[p - 1],
                )
            )
    told = [remote(tags, heard.at[p], st.at[p - 1], rt.at[p - 1], peers[p - 1]) for p in range(1, shards)]
    heard[0] = tags[...]
    for d in range(groups):
        inbox[0, d] = packed[d, pl.ds(pl.multiple_of(me * capacity, 8), capacity), :]

    per = LANES // capacity
    lane = lax.broadcasted_iota(jnp.int32, (8, LANES), 1)
    for copy in told:
        copy.wait_recv()
    for g in range(shards // per):
        both = jnp.full((8, LANES), empty, jnp.int32)
        for j in range(per):
            p = g * per + j
            turn = lax.rem((j + shards - me) * capacity, spots)
            turned = pltpu.roll(heard[p], turn, 1)[:, :LANES]
            both = jnp.where((lane >= j * capacity) & (lane < (j + 1) * capacity), turned, both)
        labels[g * groups : (g + 1) * groups, :] = both[:groups]
    for copy in moves:
        copy.wait_recv()
    for p in range(shards):
        g, j = p // per, p % per
        for d in range(groups):
            data[pl.ds((g * groups + d) * LANES + j * capacity, capacity), :] = inbox[p, d]
    for copy in asked + sent + moves + told:
        copy.wait_send()


def exchange(rows_data, owners, slot_rows, lower_rows, width):
    shards = lax.axis_size(("cx", "cy"))
    groups = lax.axis_size("rows")
    batch = rows_data.shape[0]
    capacity = -(-(2 * batch // shards) // 8) * 8
    spots = shards * capacity
    tall = -(-groups // 8) * 8
    vm = pl.BlockSpec(memory_space=pltpu.VMEM)
    f32, i32 = jnp.float32, jnp.int32
    dma = lambda n: pltpu.SemaphoreType.DMA((n,))
    many = (shards - 1) * groups
    return pl.pallas_call(
        functools.partial(exchange_kernel, capacity, lower_rows),
        out_shape=(
            jax.ShapeDtypeStruct((groups * spots, width), f32),
            jax.ShapeDtypeStruct((groups * spots // LANES, LANES), i32),
        ),
        in_specs=[vm] * 3,
        out_specs=(vm, vm),
        scratch_shapes=[
            pltpu.VMEM((8, LANES), i32),
            pltpu.VMEM((groups, 8, LANES), i32),
            pltpu.VMEM((groups, batch, width), f32),
            pltpu.VMEM((groups, spots, width), f32),
            pltpu.VMEM((shards, groups, capacity, width), f32),
            pltpu.VMEM((tall, spots), i32),
            pltpu.VMEM((shards, tall, spots), i32),
            dma(groups - 1), dma(groups - 1), dma(groups - 1), dma(groups - 1),
            dma(many), dma(many), dma(shards - 1), dma(shards - 1),
        ],
        compiler_params=pltpu.CompilerParams(
            collective_id=2, has_side_effects=True, vmem_limit_bytes=60 * 1024 * 1024
        ),
        name="exchange",
    )(rows_data, owners.reshape(1, batch), slot_rows.reshape(1, batch))


def count_columns(ids_row, rows, base, limit):
    spots = lax.broadcasted_iota(jnp.int32, (limit, LANES), 0) + base

    def step(i, total):
        line = jnp.broadcast_to(ids_row(i), (limit, LANES))
        return total + jnp.where(line == spots, 1.0, 0.0)

    total = lax.fori_loop(0, rows, step, jnp.zeros((limit, LANES), jnp.float32))
    return jnp.sum(total, axis=1, keepdims=True)


def eye(size):
    return lax.broadcasted_iota(jnp.int32, (size, size), 0) == lax.broadcasted_iota(jnp.int32, (size, size), 1)


def to_column(row, same):
    size = row.shape[1]
    return jnp.sum(jnp.where(same, jnp.broadcast_to(row, (size, size)), 0.0), axis=1, keepdims=True)


def to_row(column, same):
    size = column.shape[0]
    return jnp.sum(jnp.where(same, jnp.broadcast_to(column, (size, size)), 0.0), axis=0, keepdims=True)


TOGETHER = 4


def scatter_rows(table, source, count, label):
    def step(i, _):
        at = [i * TOGETHER + j for j in range(TOGETHER)]
        place = [label(k) for k in at]
        value = [source[pl.ds(k, 1), :] for k in at]
        held = [table[pl.ds(p, 1), :] for p in place]
        done = []
        for j in range(TOGETHER):
            total = held[j] + value[j]
            for e in range(j):
                total = total + jnp.where(place[e] == place[j], value[e], 0.0)
            done.append(total)
        for j in range(TOGETHER):
            table[pl.ds(place[j], 1), :] = done[j]
        return 0

    lax.fori_loop(0, count // TOGETHER, step, 0, unroll=4)


def local_kernel(lower_s, upper_s, lower_v, data, cent, counts, moved, news, partial, prev, now, summed, sems):
    fetch = pltpu.make_async_copy(cent, prev, sems.at[0])
    fetch.start()
    summed[...] = jnp.zeros_like(summed)
    scatter_rows(
        summed, data, data.shape[0],
        lambda k: lower_s[lax.div(k, LANES), lax.rem(k, LANES)],
    )
    partial[...] = jnp.zeros_like(partial)
    fetch.wait()
    same = eye(LANES)

    def move(b, _):
        here = pl.ds(pl.multiple_of(b * LANES, LANES), LANES)
        m = count_columns(lambda i: lower_v[pl.ds(i, 1), :], lower_v.shape[0], b * LANES, LANES)
        n = to_column(counts[pl.ds(b, 1), :], same) + m
        old = prev[here, :]
        now[here, :] = old + (summed[here, :] - m * old) / n
        news[pl.ds(b, 1), :] = to_row(n, same)
        return 0

    lax.fori_loop(0, prev.shape[0] // LANES, move, 0)
    put = pltpu.make_async_copy(now, moved, sems.at[1])
    put.start()
    scatter_rows(
        partial, now, now.shape[0],
        lambda k: upper_s[lax.div(k, LANES), lax.rem(k, LANES)],
    )
    put.wait()


def local_update(labels, ids, data, centroids, counts, slots):
    rows, width = centroids.shape
    vm = pl.BlockSpec(memory_space=pltpu.VMEM)
    sm = pl.BlockSpec(memory_space=pltpu.SMEM)
    hbm = pl.BlockSpec(memory_space=pl.ANY)
    f32 = jnp.float32
    moved, news, partial = pl.pallas_call(
        local_kernel,
        out_shape=(
            jax.ShapeDtypeStruct((rows, width), f32),
            jax.ShapeDtypeStruct((rows // LANES, LANES), f32),
            jax.ShapeDtypeStruct((slots, width), f32),
        ),
        in_specs=[sm, sm, vm, vm, hbm, vm],
        out_specs=(hbm, vm, vm),
        scratch_shapes=[
            pltpu.VMEM((rows, width), f32),
            pltpu.VMEM((rows, width), f32),
            pltpu.VMEM((rows + 8, width), f32),
            pltpu.SemaphoreType.DMA((2,)),
        ],
        compiler_params=pltpu.CompilerParams(vmem_limit_bytes=40 * 1024 * 1024),
        name="local_update",
    )(labels, ids, labels, data, centroids, counts.reshape(-1, LANES))
    return moved, news.reshape(-1), partial


def reduce_kernel(
    ys, xs, part, ids, upper, weights, out, news,
    pair, chip, a1, b1, a2, b2, seen, spread,
    s0, r0, sa1, ra1, sb1, rb1, sa2, ra2, sb2, rb2, si, ri,
):
    y = lax.axis_index("cx")
    cy = lax.axis_index("cy")
    x, core = lax.div(cy, CORES), lax.rem(cy, CORES)
    cys = xs * CORES
    shards = ys * cys
    me = y * cys + cy
    slots = part.shape[1]
    half = slots // 2
    lines = ids.shape[0]

    barrier = pltpu.get_barrier_semaphore()
    peers = []
    for d in range(1, shards):
        t = lax.rem(me + d, shards)
        peers.append({"cx": lax.div(t, cys), "cy": lax.rem(t, cys)})
    for peer in peers:
        pl.semaphore_signal(barrier, inc=1, device_id=peer, device_id_type=MESH)
    pl.semaphore_wait(barrier, shards - 1)

    def remote(src, dst, send, recv, peer):
        copy = pltpu.make_async_remote_copy(
            src_ref=src, dst_ref=dst, send_sem=send, recv_sem=recv, device_id=peer, device_id_type=MESH
        )
        copy.start()
        return copy

    offsets = [(dy, dx) for dy in range(ys) for dx in range(xs)]
    offsets.sort(key=lambda o: -((o[0] != 0) * 2 + (o[1] != 0) * 2))

    def at(dy, dx):
        return lax.rem(y + dy, ys), lax.rem(x + dx, xs)

    started = []
    first = {}
    for dy, dx in offsets:
        ty, tx = at(dy, dx)
        k = dy * xs + dx
        first[dy, dx] = remote(
            part.at[(ty * xs + tx) * CORES + 1 - core], pair.at[k], s0.at[k], r0.at[k],
            {"cx": y, "cy": x * CORES + 1 - core},
        )
    idc = [remote(ids, seen.at[d], si.at[d - 1], ri.at[d - 1], peers[d - 1]) for d in range(1, shards)]
    seen[0] = ids[...]

    ac, bc = {}, {}
    for dy, dx in offsets:
        ty, tx = at(dy, dx)
        k = dy * xs + dx
        first[dy, dx].wait_recv()
        chip[k] = part[(ty * xs + tx) * CORES + core] + pair[k]
        if dy:
            ac[dy, dx] = remote(
                chip.at[k, pl.ds(0, half)], a1.at[(dy - 1) * xs + dx],
                sa1.at[(dy - 1) * xs + dx], ra1.at[(dy - 1) * xs + dx],
                {"cx": ty, "cy": cy},
            )
        if dx:
            bc[dy, dx] = remote(
                chip.at[k, pl.ds(half, half)], b1.at[(dx - 1) * ys + dy],
                sb1.at[(dx - 1) * ys + dy], rb1.at[(dx - 1) * ys + dy],
                {"cx": y, "cy": tx * CORES + core},
            )

    a2c, b2c = {}, {}
    for dx in range(1, xs):
        for dy in range(1, ys):
            ac[dy, dx].wait_recv()
        total = chip[dx, :half]
        for dy in range(1, ys):
            total = total + a1[(dy - 1) * xs + dx]
        chip[dx, :half] = total
        a2c[dx] = remote(
            chip.at[dx, pl.ds(0, half)], a2.at[dx - 1], sa2.at[dx - 1], ra2.at[dx - 1],
            {"cx": y, "cy": lax.rem(x + dx, xs) * CORES + core},
        )
    for dy in range(1, ys):
        for dx in range(1, xs):
            bc[dy, dx].wait_recv()
        total = chip[dy * xs, half:]
        for dx in range(1, xs):
            total = total + b1[(dx - 1) * ys + dy]
        chip[dy * xs, half:] = total
        b2c[dy] = remote(
            chip.at[dy * xs, pl.ds(half, half)], b2.at[dy - 1], sb2.at[dy - 1], rb2.at[dy - 1],
            {"cx": lax.rem(y + dy, ys), "cy": cy},
        )

    for copy in idc:
        copy.wait_recv()
    block = min(LANES, slots)
    same = eye(block)
    for b in range(slots // block):
        here = pl.ds(b * block, block)
        m = count_columns(
            lambda i: seen[lax.div(i, lines), pl.ds(lax.rem(i, lines), 1), :],
            shards * lines, me * slots + b * block, block,
        )
        n = to_column(weights[b : b + 1, :], same) + m
        news[b : b + 1, :] = to_row(n, same)
        spread[here, :] = jnp.broadcast_to(n, (block, LANES))
        out[here, :] = m * upper[here, :]

    for dy in range(1, ys):
        ac[dy, 0].wait_recv()
    for dx in range(1, xs):
        bc[0, dx].wait_recv()
    for dx in range(1, xs):
        a2c[dx].wait_recv()
    for dy in range(1, ys):
        b2c[dy].wait_recv()

    def close(rows, total):
        prev = upper[rows, :]
        out[rows, :] = prev + (total - out[rows, :]) / spread[rows, :1]

    total = chip[0, :half]
    for dy in range(1, ys):
        total = total + a1[(dy - 1) * xs]
    for dx in range(1, xs):
        total = total + a2[dx - 1]
    close(pl.ds(0, half), total)
    total = chip[0, half:]
    for dx in range(1, xs):
        total = total + b1[(dx - 1) * ys]
    for dy in range(1, ys):
        total = total + b2[dy - 1]
    close(pl.ds(half, half), total)

    for group in (first.values(), idc, ac.values(), bc.values(), a2c.values(), b2c.values()):
        for copy in group:
            copy.wait_send()


def reduce_update(partial, ids, upper, weights, ys, xs):
    slots, width = upper.shape
    half = slots // 2
    block = min(LANES, slots)
    shards = ys * xs * CORES
    vm = pl.BlockSpec(memory_space=pltpu.VMEM)
    f32 = jnp.float32
    n0, na, nb = ys * xs, (ys - 1) * xs, (xs - 1) * ys
    dma = lambda n: pltpu.SemaphoreType.DMA((n,))
    new_upper, news = pl.pallas_call(
        functools.partial(reduce_kernel, ys, xs),
        out_shape=(
            jax.ShapeDtypeStruct((slots, width), f32),
            jax.ShapeDtypeStruct((slots // block, block), f32),
        ),
        in_specs=[vm] * 4,
        out_specs=(vm, vm),
        scratch_shapes=[
            pltpu.VMEM((n0, slots, width), f32),
            pltpu.VMEM((n0, slots, width), f32),
            pltpu.VMEM((na, half, width), f32),
            pltpu.VMEM((nb, half, width), f32),
            pltpu.VMEM((xs - 1, half, width), f32),
            pltpu.VMEM((ys - 1, half, width), f32),
            pltpu.VMEM((shards,) + ids.shape, jnp.int32),
            pltpu.VMEM((slots, LANES), f32),
            dma(n0), dma(n0), dma(na), dma(na), dma(nb), dma(nb),
            dma(xs - 1), dma(xs - 1), dma(ys - 1), dma(ys - 1),
            dma(shards - 1), dma(shards - 1),
        ],
        compiler_params=pltpu.CompilerParams(
            collective_id=1, has_side_effects=True, vmem_limit_bytes=60 * 1024 * 1024
        ),
        name="reduce_update",
    )(
        partial.reshape(shards, slots, width),
        ids,
        upper,
        weights.reshape(-1, block),
    )
    return new_upper, news.reshape(-1)


def body(
    rows_data, owner_rows, slot_rows, centroids, counts, owner_cent, slot_cent, upper, upper_counts
):
    ys, xs = lax.axis_size("cx"), lax.axis_size("cy") // CORES
    upper_rows = upper.shape[0]
    ids = (owner_cent[:, 0] * upper_rows + slot_cent).reshape(-1, LANES)
    data, labels = exchange(rows_data, owner_rows, slot_rows, *centroids.shape)
    moved, new_counts, partial = local_update(
        labels, ids, data, centroids, counts, upper_rows * ys * xs * CORES
    )
    new_upper, new_upper_counts = reduce_update(partial, ids, upper, upper_counts, ys, xs)
    return (moved, new_counts, new_upper, new_upper_counts)


def solution(mesh):
    placed = (
        P(("rows", "cx", "cy"), None),
        P(("rows", "cx", "cy"), None),
        P(("rows", "cx", "cy")),
        P(("cx", "cy"), "rows"),
        P(("cx", "cy")),
        P(("cx", "cy"), None),
        P(("cx", "cy")),
        P(("cx", "cy"), "rows"),
        P(("cx", "cy")),
    )
    return jax.shard_map(
        body,
        mesh=mesh,
        in_specs=placed,
        out_specs=(
            P(("cx", "cy"), "rows"),
            P(("cx", "cy")),
            P(("cx", "cy"), "rows"),
            P(("cx", "cy")),
        ),
        check_vma=False,
    )
```

```python
import functools

import jax
import jax.numpy as jnp
from jax import lax
from jax.experimental import pallas as pl
from jax.experimental.pallas import tpu as pltpu
from jax.sharding import PartitionSpec as P

MESH = pl.DeviceIdType.MESH
LANES = 128
CORES = 2


def exchange_kernel(
    capacity, empty, rows_ref, owner_ref, slot_ref, data, labels,
    info, mine, slabs, packed, inbox, tags, heard,
    si, ri, ss, rs, sp, rp, st, rt,
):
    groups, batch, width = slabs.shape
    shards = inbox.shape[0]
    spots = shards * capacity
    z = lax.axis_index("rows")
    cys = lax.axis_size("cy")
    me = lax.axis_index("cx") * cys + lax.axis_index("cy")

    info[...] = jnp.full_like(info, -1)
    info[0:1, :batch] = owner_ref[...]
    info[1:2, :batch] = slot_ref[...]
    tags[...] = jnp.full_like(tags, empty)

    barrier = pltpu.get_barrier_semaphore()
    mates = [{"rows": lax.rem(z + d, groups)} for d in range(1, groups)]
    peers = []
    for d in range(1, shards):
        t = lax.rem(me + d, shards)
        peers.append({"cx": lax.div(t, cys), "cy": lax.rem(t, cys)})
    for peer in mates + peers:
        pl.semaphore_signal(barrier, inc=1, device_id=peer, device_id_type=MESH)
    pl.semaphore_wait(barrier, groups - 1 + shards - 1)

    def remote(src, dst, send, recv, peer):
        copy = pltpu.make_async_remote_copy(
            src_ref=src, dst_ref=dst, send_sem=send, recv_sem=recv, device_id=peer, device_id_type=MESH
        )
        copy.start()
        return copy

    def columns(group):
        return pl.ds(pl.multiple_of(group * width, width), width)

    asked = [remote(info, mine.at[d], si.at[d - 1], ri.at[d - 1], mates[d - 1]) for d in range(1, groups)]
    sent = [
        remote(
            rows_ref.at[:, columns(mates[d - 1]["rows"])], slabs.at[d],
            ss.at[d - 1], rs.at[d - 1], mates[d - 1],
        )
        for d in range(1, groups)
    ]
    mine[0] = info[...]
    slabs[0] = rows_ref[:, columns(z)]

    bf16, f32 = jnp.bfloat16, jnp.float32
    up = lax.broadcasted_iota(jnp.int32, (LANES, LANES), 0)
    across = lax.broadcasted_iota(jnp.int32, (LANES, LANES), 1)
    before = jnp.where(up < across, 1.0, 0.0).astype(bf16)
    shard_of = lax.broadcasted_iota(jnp.int32, (shards, LANES), 0)
    spot_of = lax.broadcasted_iota(jnp.int32, (spots, LANES), 0)
    line = lax.broadcasted_iota(jnp.int32, (8, LANES), 0)
    moves = []
    for d in range(groups):
        if d:
            asked[d - 1].wait_recv()
        owner, slot = mine[d, 0:1, :], mine[d, 1:2, :]
        named = jnp.where(jnp.broadcast_to(owner, (shards, LANES)) == shard_of, 1.0, 0.0)
        earlier = jnp.dot(named.astype(bf16), before, preferred_element_type=f32)
        position = jnp.sum(named * earlier, axis=0, keepdims=True).astype(jnp.int32)
        target = jnp.where(owner >= 0, owner * capacity + position, -1)
        pick = jnp.where(jnp.broadcast_to(target, (spots, LANES)) == spot_of, 1.0, 0.0).astype(bf16)
        high = jnp.broadcast_to(lax.shift_right_arithmetic(slot, 7), (8, LANES))
        low = jnp.broadcast_to(slot & 127, (8, LANES))
        code = jnp.where(line == 0, high, jnp.where(line == 1, low, 1)).astype(f32).astype(bf16)
        found = lax.dot_general(code, pick, (((1,), (1,)), ((), ())), preferred_element_type=f32)
        tag = (found[0:1] * 128.0 + found[1:2]).astype(jnp.int32)
        tags[d : d + 1, :] = jnp.where(found[2:3] > 0.5, tag, empty)
        if d:
            sent[d - 1].wait_recv()
        slab = slabs[d]
        first = slab.astype(bf16)
        left = slab - first.astype(f32)
        second = left.astype(bf16)
        third = (left - second.astype(f32)).astype(bf16)
        chosen = pick[:, :batch]
        total = jnp.dot(chosen, third, preferred_element_type=f32)
        total = total + jnp.dot(chosen, second, preferred_element_type=f32)
        packed[d] = total + jnp.dot(chosen, first, preferred_element_type=f32)
        for p in range(1, shards):
            t = lax.rem(me + p, shards)
            k = (p - 1) * groups + d
            moves.append(
                remote(
                    packed.at[d, pl.ds(pl.multiple_of(t * capacity, 8), capacity)], inbox.at[p, d],
                    sp.at[k], rp.at[k], peers[p - 1],
                )
            )
    told = [remote(tags, heard.at[p], st.at[p - 1], rt.at[p - 1], peers[p - 1]) for p in range(1, shards)]
    heard[0] = tags[...]
    for d in range(groups):
        inbox[0, d] = packed[d, pl.ds(pl.multiple_of(me * capacity, 8), capacity), :]

    per = LANES // capacity
    lane = lax.broadcasted_iota(jnp.int32, (8, LANES), 1)
    for copy in told:
        copy.wait_recv()
    for g in range(shards // per):
        both = jnp.full((8, LANES), empty, jnp.int32)
        for j in range(per):
            p = g * per + j
            turn = lax.rem((j + shards - me) * capacity, spots)
            turned = pltpu.roll(heard[p], turn, 1)[:, :LANES]
            both = jnp.where((lane >= j * capacity) & (lane < (j + 1) * capacity), turned, both)
        labels[g * groups : (g + 1) * groups, :] = both[:groups]
    for copy in moves:
        copy.wait_recv()
    for p in range(shards):
        g, j = p // per, p % per
        for d in range(groups):
            data[pl.ds((g * groups + d) * LANES + j * capacity, capacity), :] = inbox[p, d]
    for copy in asked + sent + moves + told:
        copy.wait_send()


def exchange(rows_data, owners, slot_rows, lower_rows, width):
    shards = lax.axis_size(("cx", "cy"))
    groups = lax.axis_size("rows")
    batch = rows_data.shape[0]
    capacity = -(-(2 * batch // shards) // 8) * 8
    spots = shards * capacity
    tall = -(-groups // 8) * 8
    vm = pl.BlockSpec(memory_space=pltpu.VMEM)
    f32, i32 = jnp.float32, jnp.int32
    dma = lambda n: pltpu.SemaphoreType.DMA((n,))
    many = (shards - 1) * groups
    return pl.pallas_call(
        functools.partial(exchange_kernel, capacity, lower_rows),
        out_shape=(
            jax.ShapeDtypeStruct((groups * spots, width), f32),
            jax.ShapeDtypeStruct((groups * spots // LANES, LANES), i32),
        ),
        in_specs=[vm] * 3,
        out_specs=(vm, vm),
        scratch_shapes=[
            pltpu.VMEM((8, LANES), i32),
            pltpu.VMEM((groups, 8, LANES), i32),
            pltpu.VMEM((groups, batch, width), f32),
            pltpu.VMEM((groups, spots, width), f32),
            pltpu.VMEM((shards, groups, capacity, width), f32),
            pltpu.VMEM((tall, spots), i32),
            pltpu.VMEM((shards, tall, spots), i32),
            dma(groups - 1), dma(groups - 1), dma(groups - 1), dma(groups - 1),
            dma(many), dma(many), dma(shards - 1), dma(shards - 1),
        ],
        compiler_params=pltpu.CompilerParams(
            collective_id=2, has_side_effects=True, vmem_limit_bytes=16 * 1024 * 1024
        ),
        name="exchange",
    )(rows_data, owners.reshape(1, batch), slot_rows.reshape(1, batch))


def count_columns(ids_row, rows, base, limit):
    spots = lax.broadcasted_iota(jnp.int32, (limit, LANES), 0) + base

    def step(i, total):
        line = jnp.broadcast_to(ids_row(i), (limit, LANES))
        return total + jnp.where(line == spots, 1.0, 0.0)

    total = lax.fori_loop(0, rows, step, jnp.zeros((limit, LANES), jnp.float32))
    return jnp.sum(total, axis=1, keepdims=True)


def eye(size):
    return lax.broadcasted_iota(jnp.int32, (size, size), 0) == lax.broadcasted_iota(jnp.int32, (size, size), 1)


def to_column(row, same):
    size = row.shape[1]
    return jnp.sum(jnp.where(same, jnp.broadcast_to(row, (size, size)), 0.0), axis=1, keepdims=True)


def to_row(column, same):
    size = column.shape[0]
    return jnp.sum(jnp.where(same, jnp.broadcast_to(column, (size, size)), 0.0), axis=0, keepdims=True)


def scatter_rows(tables, source, count, ids):
    many = len(tables)
    steps = LANES // many

    def step(i, _):
        line, first = lax.div(i, steps), lax.rem(i, steps) * many
        for j, table in enumerate(tables):
            table[pl.ds(ids[line, first + j], 1), :] += source[pl.ds(i * many + j, 1), :]
        return 0

    lax.fori_loop(0, count // many, step, 0, unroll=8)


def local_kernel(
    lower_s, upper_s, lower_v, data, cent, counts, moved, news, partial, now, sum0, sum1, t1, t2, t3, sems
):
    for table in (sum0, sum1, partial, t1, t2, t3):
        table[...] = jnp.zeros_like(table)
    scatter_rows((sum0, sum1), data, data.shape[0], lower_s)
    same = eye(LANES)

    def move(b, _):
        here = pl.ds(pl.multiple_of(b * LANES, LANES), LANES)
        m = count_columns(lambda i: lower_v[pl.ds(i, 1), :], lower_v.shape[0], b * LANES, LANES)
        n = to_column(counts[pl.ds(b, 1), :], same) + m
        old = cent[here, :]
        now[here, :] = old + (sum0[here, :] + sum1[here, :] - m * old) / n
        news[pl.ds(b, 1), :] = to_row(n, same)
        return 0

    lax.fori_loop(0, cent.shape[0] // LANES, move, 0)
    put = pltpu.make_async_copy(now, moved, sems.at[0])
    put.start()
    scatter_rows((partial, t1, t2, t3), now, now.shape[0], upper_s)

    def join(b, _):
        here = pl.ds(pl.multiple_of(b * LANES, LANES), LANES)
        partial[here, :] = (partial[here, :] + t1[here, :]) + (t2[here, :] + t3[here, :])
        return 0

    lax.fori_loop(0, partial.shape[0] // LANES, join, 0)
    put.wait()


def local_update(labels, ids, data, centroids, counts, slots):
    rows, width = centroids.shape
    vm = pl.BlockSpec(memory_space=pltpu.VMEM)
    sm = pl.BlockSpec(memory_space=pltpu.SMEM)
    hbm = pl.BlockSpec(memory_space=pl.ANY)
    f32 = jnp.float32
    moved, news, partial = pl.pallas_call(
        local_kernel,
        out_shape=(
            jax.ShapeDtypeStruct((rows, width), f32),
            jax.ShapeDtypeStruct((rows // LANES, LANES), f32),
            jax.ShapeDtypeStruct((slots, width), f32),
        ),
        in_specs=[sm, sm, vm, vm, vm, vm],
        out_specs=(hbm, vm, vm),
        scratch_shapes=[
            pltpu.VMEM((rows, width), f32),
            pltpu.VMEM((rows + 8, width), f32),
            pltpu.VMEM((rows + 8, width), f32),
            pltpu.VMEM((slots, width), f32),
            pltpu.VMEM((slots, width), f32),
            pltpu.VMEM((slots, width), f32),
            pltpu.SemaphoreType.DMA((1,)),
        ],
        compiler_params=pltpu.CompilerParams(vmem_limit_bytes=32 * 1024 * 1024),
        name="local_update",
    )(labels, ids, labels, data, centroids, counts.reshape(-1, LANES))
    return moved, news.reshape(-1), partial


def reduce_kernel(
    ys, xs, part, ids, out, members,
    pair, chip, a1, b1, a2, b2, seen,
    s0, r0, sa1, ra1, sb1, rb1, sa2, ra2, sb2, rb2, si, ri,
):
    y = lax.axis_index("cx")
    cy = lax.axis_index("cy")
    x, core = lax.div(cy, CORES), lax.rem(cy, CORES)
    cys = xs * CORES
    shards = ys * cys
    me = y * cys + cy
    slots = part.shape[1]
    half = slots // 2
    lines = ids.shape[0]

    barrier = pltpu.get_barrier_semaphore()
    peers = []
    for d in range(1, shards):
        t = lax.rem(me + d, shards)
        peers.append({"cx": lax.div(t, cys), "cy": lax.rem(t, cys)})
    for peer in peers:
        pl.semaphore_signal(barrier, inc=1, device_id=peer, device_id_type=MESH)
    pl.semaphore_wait(barrier, shards - 1)

    def remote(src, dst, send, recv, peer):
        copy = pltpu.make_async_remote_copy(
            src_ref=src, dst_ref=dst, send_sem=send, recv_sem=recv, device_id=peer, device_id_type=MESH
        )
        copy.start()
        return copy

    offsets = [(dy, dx) for dy in range(ys) for dx in range(xs)]
    offsets.sort(key=lambda o: -((o[0] != 0) * 2 + (o[1] != 0) * 2))

    def at(dy, dx):
        return lax.rem(y + dy, ys), lax.rem(x + dx, xs)

    started = []
    first = {}
    for dy, dx in offsets:
        ty, tx = at(dy, dx)
        k = dy * xs + dx
        first[dy, dx] = remote(
            part.at[(ty * xs + tx) * CORES + 1 - core], pair.at[k], s0.at[k], r0.at[k],
            {"cx": y, "cy": x * CORES + 1 - core},
        )
    idc = [remote(ids, seen.at[d], si.at[d - 1], ri.at[d - 1], peers[d - 1]) for d in range(1, shards)]
    seen[0] = ids[...]

    ac, bc = {}, {}
    for dy, dx in offsets:
        ty, tx = at(dy, dx)
        k = dy * xs + dx
        first[dy, dx].wait_recv()
        chip[k] = part[(ty * xs + tx) * CORES + core] + pair[k]
        if dy:
            ac[dy, dx] = remote(
                chip.at[k, pl.ds(0, half)], a1.at[(dy - 1) * xs + dx],
                sa1.at[(dy - 1) * xs + dx], ra1.at[(dy - 1) * xs + dx],
                {"cx": ty, "cy": cy},
            )
        if dx:
            bc[dy, dx] = remote(
                chip.at[k, pl.ds(half, half)], b1.at[(dx - 1) * ys + dy],
                sb1.at[(dx - 1) * ys + dy], rb1.at[(dx - 1) * ys + dy],
                {"cx": y, "cy": tx * CORES + core},
            )

    a2c, b2c = {}, {}
    for dx in range(1, xs):
        for dy in range(1, ys):
            ac[dy, dx].wait_recv()
        total = chip[dx, :half]
        for dy in range(1, ys):
            total = total + a1[(dy - 1) * xs + dx]
        chip[dx, :half] = total
        a2c[dx] = remote(
            chip.at[dx, pl.ds(0, half)], a2.at[dx - 1], sa2.at[dx - 1], ra2.at[dx - 1],
            {"cx": y, "cy": lax.rem(x + dx, xs) * CORES + core},
        )
    for dy in range(1, ys):
        for dx in range(1, xs):
            bc[dy, dx].wait_recv()
        total = chip[dy * xs, half:]
        for dx in range(1, xs):
            total = total + b1[(dx - 1) * ys + dy]
        chip[dy * xs, half:] = total
        b2c[dy] = remote(
            chip.at[dy * xs, pl.ds(half, half)], b2.at[dy - 1], sb2.at[dy - 1], rb2.at[dy - 1],
            {"cx": lax.rem(y + dy, ys), "cy": cy},
        )

    for copy in idc:
        copy.wait_recv()
    block = min(LANES, slots)
    for b in range(slots // block):
        here = pl.ds(b * block, block)
        m = count_columns(
            lambda i: seen[lax.div(i, lines), pl.ds(lax.rem(i, lines), 1), :],
            shards * lines, me * slots + b * block, block,
        )
        members[here, :] = jnp.broadcast_to(m, (block, LANES))

    for dy in range(1, ys):
        ac[dy, 0].wait_recv()
    for dx in range(1, xs):
        bc[0, dx].wait_recv()
    for dx in range(1, xs):
        a2c[dx].wait_recv()
    for dy in range(1, ys):
        b2c[dy].wait_recv()

    total = chip[0, :half]
    for dy in range(1, ys):
        total = total + a1[(dy - 1) * xs]
    for dx in range(1, xs):
        total = total + a2[dx - 1]
    out[:half, :] = total
    total = chip[0, half:]
    for dx in range(1, xs):
        total = total + b1[(dx - 1) * ys]
    for dy in range(1, ys):
        total = total + b2[dy - 1]
    out[half:, :] = total

    for group in (first.values(), idc, ac.values(), bc.values(), a2c.values(), b2c.values()):
        for copy in group:
            copy.wait_send()


def finish_kernel(total, members, upper, weights, out, news):
    lines, block = weights.shape
    same = eye(block)
    for b in range(lines):
        here = pl.ds(b * block, block)
        m = members[here, :1]
        n = to_column(weights[b : b + 1, :], same) + m
        prev = upper[here, :]
        out[here, :] = prev + (total[here, :] - m * prev) / n
        news[b : b + 1, :] = to_row(n, same)


def reduce_update(partial, ids, upper, weights, ys, xs):
    slots, width = upper.shape
    half = slots // 2
    block = min(LANES, slots)
    shards = ys * xs * CORES
    vm = pl.BlockSpec(memory_space=pltpu.VMEM)
    f32 = jnp.float32
    n0, na, nb = ys * xs, (ys - 1) * xs, (xs - 1) * ys
    dma = lambda n: pltpu.SemaphoreType.DMA((n,))
    total, members = pl.pallas_call(
        functools.partial(reduce_kernel, ys, xs),
        out_shape=(
            jax.ShapeDtypeStruct((slots, width), f32),
            jax.ShapeDtypeStruct((slots, LANES), f32),
        ),
        in_specs=[vm] * 2,
        out_specs=(vm, vm),
        scratch_shapes=[
            pltpu.VMEM((n0, slots, width), f32),
            pltpu.VMEM((n0, slots, width), f32),
            pltpu.VMEM((na, half, width), f32),
            pltpu.VMEM((nb, half, width), f32),
            pltpu.VMEM((xs - 1, half, width), f32),
            pltpu.VMEM((ys - 1, half, width), f32),
            pltpu.VMEM((shards,) + ids.shape, jnp.int32),
            dma(n0), dma(n0), dma(na), dma(na), dma(nb), dma(nb),
            dma(xs - 1), dma(xs - 1), dma(ys - 1), dma(ys - 1),
            dma(shards - 1), dma(shards - 1),
        ],
        compiler_params=pltpu.CompilerParams(
            collective_id=1, has_side_effects=True, vmem_limit_bytes=20 * 1024 * 1024
        ),
        name="reduce_update",
    )(
        partial.reshape(shards, slots, width),
        ids,
    )
    new_upper, news = pl.pallas_call(
        finish_kernel,
        out_shape=(
            jax.ShapeDtypeStruct((slots, width), f32),
            jax.ShapeDtypeStruct((slots // block, block), f32),
        ),
        in_specs=[vm] * 4,
        out_specs=(vm, vm),
        compiler_params=pltpu.CompilerParams(vmem_limit_bytes=8 * 1024 * 1024),
        name="finish",
    )(total, members, upper, weights.reshape(-1, block))
    return new_upper, news.reshape(-1)


def body(
    rows_data, owner_rows, slot_rows, centroids, counts, owner_cent, slot_cent, upper, upper_counts
):
    ys, xs = lax.axis_size("cx"), lax.axis_size("cy") // CORES
    upper_rows = upper.shape[0]
    ids = (owner_cent[:, 0] * upper_rows + slot_cent).reshape(-1, LANES)
    data, labels = exchange(rows_data, owner_rows, slot_rows, *centroids.shape)
    moved, new_counts, partial = local_update(
        labels, ids, data, centroids, counts, upper_rows * ys * xs * CORES
    )
    new_upper, new_upper_counts = reduce_update(partial, ids, upper, upper_counts, ys, xs)
    return (moved, new_counts, new_upper, new_upper_counts)


def solution(mesh):
    placed = (
        P(("rows", "cx", "cy"), None),
        P(("rows", "cx", "cy"), None),
        P(("rows", "cx", "cy")),
        P(("cx", "cy"), "rows"),
        P(("cx", "cy")),
        P(("cx", "cy"), None),
        P(("cx", "cy")),
        P(("cx", "cy"), "rows"),
        P(("cx", "cy")),
    )
    return jax.shard_map(
        body,
        mesh=mesh,
        in_specs=placed,
        out_specs=(
            P(("cx", "cy"), "rows"),
            P(("cx", "cy")),
            P(("cx", "cy"), "rows"),
            P(("cx", "cy")),
        ),
        check_vma=False,
    )
```
